32 devices in a mesh: row: 4 (over y, core), col: 8 (over z, x).
Axes of the slice: x: 2, y: 2, z: 4, core: 2. Of those that a mesh axis runs over, the one named last changes fastest.
Arguments:
- adjacency: int32 [8192, 8192], P('row', 'col'), may hold values from 0 to 1, as said below
Outputs:
- closure: bfloat16 [8192, 8192], P('row', 'col')
The draws below stay inside these ranges and needn't reach their ends.
Inputs may be any that keep to these rules, and one draw needn't show every extreme that they name: `adjacency`: every entry is 0 or 1; there is no bound on the number of ones in a row, a column or a block, and their share differs widely between rows and between columns.
All inputs are finite; a program needn't handle non-finite values.
Results may differ from the reference program's by a relative error of at most 0.001.
Values may be sent and summed in bfloat16 or wider, within the bound.
A program may use at most 192 MiB of HBM per device.

```python
import math
import jax
import jax.numpy as jnp
from jax import lax

PANEL = 512
PANELS = 4
ROWS = 8192
VERTS = 8192


def draw_adjacency(key, part):
    window = PANELS * PANEL
    scale_top = 1 << 20
    plain_level = scale_top // math.isqrt(window)
    sparse_level = scale_top // window
    dense_level = scale_top // 2
    key_hubs, key_levels, key_dense, key_entries = jax.random.split(jax.random.fold_in(key, 7), 4)
    hub_flags = (jax.random.randint(key_hubs, (window,), 0, 3, dtype=jnp.int32) < 2).astype(jnp.int32)
    column_hub = jnp.concatenate([hub_flags, jnp.zeros((VERTS - window,), jnp.int32)])
    row_hub = jnp.concatenate([hub_flags, jnp.zeros((ROWS - window,), jnp.int32)])
    row_ids = jnp.arange(ROWS, dtype=jnp.int32)
    levels = jax.random.randint(key_levels, (ROWS,), 0, 3, dtype=jnp.int32)
    row_plain = jnp.where(levels == 0, plain_level // 2, jnp.where(levels == 1, plain_level, plain_level * 2))
    dense_pick = jax.random.randint(key_dense, (ROWS,), 0, 16, dtype=jnp.int32)
    dense_row = (dense_pick == 0) & (row_ids >= window) | (row_hub == 1)
    on_plain = jnp.where(dense_row, dense_level, row_plain).astype(jnp.int32)
    threshold = jnp.where(column_hub[None, :] == 1, jnp.int32(sparse_level), on_plain[:, None])
    entry_draws = jax.random.randint(key_entries, (ROWS, VERTS), 0, scale_top, dtype=jnp.int32)
    return (entry_draws < threshold).astype(jnp.int32)


def setup_inputs(seed: int = 0) -> dict:
    streams_of = jax.random.split(jax.random.key(seed), 2)
    return {
        "adjacency": draw_adjacency(jax.random.fold_in(streams_of[1], 71), 0),
    }


def reference(adjacency):
    window_cols = PANELS * PANEL
    right_rows = adjacency[:window_cols].astype(jnp.float32)
    block = math.gcd(ROWS, 2048)
    blocks = adjacency.reshape(ROWS // block, block, VERTS)

    def close_rows(rows_int):
        counts = jnp.dot(rows_int[:, :window_cols].astype(jnp.float32), right_rows,
                         precision=lax.Precision.HIGHEST, preferred_element_type=jnp.float32)
        return jnp.where(counts > 0.5, 1.0, rows_int.astype(jnp.float32)).astype(jnp.bfloat16)

    return lax.map(close_rows, blocks).reshape(ROWS, VERTS)
```

```python
import functools

import jax
import jax.numpy as jnp
from jax import lax
from jax.experimental import pallas as pl
from jax.experimental.pallas import tpu as pltpu
from jax.sharding import PartitionSpec as P

PANEL = 512
PANELS = 4

CHUNK = 32
RIGHT = 64
GROUP = 256
TILE = 256
PER_STEP = 2
MESH = pl.DeviceIdType.MESH


def lag_of(row):
    return (5 * row) // 2


def kernel(n_rows, n_cols, window, adj_hbm, out, adj, left, right,
           adj_sem, z_send, z_recv, x_send, x_recv, r_send, r_recv):
    block_rows, block_cols = adj.shape
    holders = left.shape[0]
    stages = n_cols // holders
    n_chunks = block_rows // CHUNK
    n_adj = block_rows // RIGHT
    n_right = window // RIGHT
    n_groups = block_rows // GROUP
    n_tiles = block_cols // TILE
    units = n_groups * n_tiles
    per_group = GROUP // CHUNK

    r = lax.axis_index("row")
    c = lax.axis_index("col")
    hi = c // holders
    lo = lax.rem(c, holders)
    lag = lag_of(r)

    def adj_copy(i):
        rows = pl.ds(pl.multiple_of(i * RIGHT, RIGHT), RIGHT)
        return pltpu.make_async_copy(adj_hbm.at[rows], adj.at[rows], adj_sem.at[i])

    def chunk(j):
        return pl.ds(pl.multiple_of(j * CHUNK, CHUNK), CHUNK)

    def z_copy(j):
        part = left.at[lo, chunk(j)]
        return pltpu.make_async_remote_copy(
            src_ref=part, dst_ref=part, send_sem=z_send.at[j], recv_sem=z_recv.at[j],
            device_id={"col": c + holders}, device_id_type=MESH)

    def x_copy(d, j):
        part = left.at[lo, chunk(j)]
        peer = hi * holders + lax.rem(lo + d, holders)
        return pltpu.make_async_remote_copy(
            src_ref=part, dst_ref=part, send_sem=x_send.at[d - 1, j], recv_sem=x_recv.at[d - 1, j],
            device_id={"col": peer}, device_id_type=MESH)

    def x_arrival(d, j):
        part = left.at[lax.rem(lo + holders - d, holders), chunk(j)]
        peer = hi * holders + lax.rem(lo + holders - d, holders)
        return pltpu.make_async_remote_copy(
            src_ref=part, dst_ref=part, send_sem=x_send.at[d - 1, j], recv_sem=x_recv.at[d - 1, j],
            device_id={"col": peer}, device_id_type=MESH)

    def r_rows(i):
        return pl.ds(pl.multiple_of(i * RIGHT, RIGHT), RIGHT)

    def r_copy(i):
        part = right.at[r_rows(i)]
        return pltpu.make_async_remote_copy(
            src_ref=part, dst_ref=part, send_sem=r_send.at[i], recv_sem=r_recv.at[i],
            device_id={"row": r + 1}, device_id_type=MESH)

    @pl.loop(0, n_adj)
    def _(i):
        adj_copy(i).start()

    barrier = pltpu.get_barrier_semaphore()

    def greet(where):
        pl.semaphore_signal(barrier, inc=1, device_id=where, device_id_type=MESH)

    @pl.when(hi > 0)
    def _():
        greet({"col": c - holders})

    @pl.when(hi < stages - 1)
    def _():
        greet({"col": c + holders})

    for d in range(1, holders):
        greet({"col": hi * holders + lax.rem(lo + d, holders)})

    @pl.when(r > 0)
    def _():
        greet({"row": r - 1})

    @pl.when(r < n_rows - 1)
    def _():
        greet({"row": r + 1})

    def convert_left(j):
        left[lo, chunk(j), :] = adj[chunk(j), :].astype(jnp.bfloat16)

    def convert_right(i):
        right[r_rows(i), :] = adj[r_rows(i), :].astype(jnp.bfloat16)

    adj_copy(0).wait()

    @pl.when(hi == 0)
    def _():
        convert_left(0)

    @pl.when(r == 0)
    def _():
        convert_right(0)

    known = ((hi > 0).astype(jnp.int32) + (hi < stages - 1).astype(jnp.int32) + (holders - 1)
             + (r > 0).astype(jnp.int32) + (r < n_rows - 1).astype(jnp.int32))
    pl.semaphore_wait(barrier, known)

    def step(j):
        @pl.when(j + 1 < n_adj)
        def _():
            adj_copy(j + 1).wait()

        @pl.when((hi == 0) & (j + 1 < n_chunks))
        def _():
            convert_left(j + 1)

        @pl.when((r == 0) & (j + 1 < n_right))
        def _():
            convert_right(j + 1)

        @pl.when(hi > 0)
        def _():
            z_copy(j).wait_recv()

        @pl.when(hi < stages - 1)
        def _():
            z_copy(j).start()

        for d in range(1, holders):
            x_copy(d, j).start()

        i = j - lag

        @pl.when((i >= 0) & (i < n_right))
        def _():
            @pl.when(r > 0)
            def _():
                r_copy(i).wait_recv()

            @pl.when(r < n_rows - 1)
            def _():
                r_copy(i).start()

    def compute(u):
        g = u // n_tiles
        t = lax.rem(u, n_tiles)

        @pl.when(t == 0)
        def _():
            for d in range(1, holders):
                @pl.loop(0, per_group)
                def _(k):
                    x_arrival(d, g * per_group + k).wait_recv()

        rows = pl.ds(pl.multiple_of(g * GROUP, GROUP), GROUP)
        cols = pl.ds(pl.multiple_of(t * TILE, TILE), TILE)
        counts = jnp.zeros((GROUP, TILE), jnp.float32)
        for h in range(holders):
            counts += jnp.dot(left[h, rows, :], right[h * block_cols:(h + 1) * block_cols, cols],
                              preferred_element_type=jnp.float32)
        out[rows, cols] = jnp.where(counts > 0.5, 1, adj[rows, cols]).astype(out.dtype)

    body_units = units - n_tiles
    ready = n_right - 1 + lag_of(n_rows - 1)
    first = min(n_chunks, max(ready, n_chunks - 2 - -(-body_units // PER_STEP)))
    done = min(body_units, PER_STEP * (n_chunks - first))
    done -= done % PER_STEP

    @pl.loop(0, first)
    def _(j):
        step(j)

    @pl.loop(first, n_chunks)
    def _(j):
        step(j)
        for p in range(PER_STEP):
            u = (j - first) * PER_STEP + p

            @pl.when(u < done)
            def _():
                compute(u)

    @pl.loop(n_chunks, max(n_chunks, ready + 1))
    def _(j):
        i = j - lag

        @pl.when((i >= 0) & (i < n_right))
        def _():
            @pl.when(r > 0)
            def _():
                r_copy(i).wait_recv()

            @pl.when(r < n_rows - 1)
            def _():
                r_copy(i).start()

    @pl.loop(done, units)
    def _(u):
        compute(u)

    @pl.loop(0, n_chunks)
    def _(j):
        @pl.when(hi < stages - 1)
        def _():
            z_copy(j).wait_send()

        for d in range(1, holders):
            x_copy(d, j).wait_send()

    @pl.when(r < n_rows - 1)
    def _():
        @pl.loop(0, n_right)
        def _(i):
            r_copy(i).wait_send()


def per_device(n_rows, n_cols, adjacency):
    block_rows, block_cols = adjacency.shape
    window = PANELS * PANEL
    holders = window // block_cols
    n_chunks = block_rows // CHUNK
    dma = pltpu.SemaphoreType.DMA
    closed = pl.pallas_call(
        functools.partial(kernel, n_rows, n_cols, window),
        out_shape=jax.ShapeDtypeStruct((block_rows, block_cols), jnp.int8),
        in_specs=[pl.BlockSpec(memory_space=pl.ANY)],
        out_specs=pl.BlockSpec(memory_space=pltpu.VMEM),
        scratch_shapes=[
            pltpu.VMEM((block_rows, block_cols), jnp.int32),
            pltpu.VMEM((holders, block_rows, block_cols), jnp.bfloat16),
            pltpu.VMEM((window, block_cols), jnp.bfloat16),
            dma((block_rows // RIGHT,)),
            dma((n_chunks,)),
            dma((n_chunks,)),
            dma((holders - 1, n_chunks)),
            dma((holders - 1, n_chunks)),
            dma((window // RIGHT,)),
            dma((window // RIGHT,)),
        ],
        compiler_params=pltpu.CompilerParams(
            collective_id=0, has_side_effects=True, vmem_limit_bytes=58 * 1024 * 1024),
    )(adjacency)
    return closed.astype(jnp.bfloat16)


def solution(mesh):
    spec = P("row", "col")
    return jax.shard_map(
        functools.partial(per_device, mesh.shape["row"], mesh.shape["col"]),
        mesh=mesh, in_specs=(spec,), out_specs=spec, check_vma=False)
```

```python
import functools

import jax
import jax.numpy as jnp
from jax import lax
from jax.experimental import pallas as pl
from jax.experimental.pallas import tpu as pltpu
from jax.sharding import PartitionSpec as P

PANEL = 512
PANELS = 4

CHUNK = 32
RIGHT = 64
GROUP = 256
TILE = 256
PER_STEP = 2
MESH = pl.DeviceIdType.MESH


def lag_of(row):
    return (5 * row) // 2


def kernel(n_rows, n_cols, window, adj_hbm, out, adj, left, right,
           adj_sem, z_send, z_recv, x_send, x_recv, r_send, r_recv):
    block_rows, block_cols = adj.shape
    holders = left.shape[0]
    stages = n_cols // holders
    n_chunks = block_rows // CHUNK
    n_adj = block_rows // RIGHT
    n_right = window // RIGHT
    n_groups = block_rows // GROUP
    n_tiles = block_cols // TILE
    units = n_groups * n_tiles
    per_group = GROUP // CHUNK

    r = lax.axis_index("row")
    c = lax.axis_index("col")
    hi = c // holders
    lo = lax.rem(c, holders)
    lag = lag_of(r)

    def adj_copy(i):
        rows = pl.ds(pl.multiple_of(i * RIGHT, RIGHT), RIGHT)
        return pltpu.make_async_copy(adj_hbm.at[rows], adj.at[rows], adj_sem.at[i])

    def chunk(j):
        return pl.ds(pl.multiple_of(j * CHUNK, CHUNK), CHUNK)

    def z_copy(j):
        part = left.at[lo, chunk(j)]
        return pltpu.make_async_remote_copy(
            src_ref=part, dst_ref=part, send_sem=z_send, recv_sem=z_recv.at[j],
            device_id={"col": c + holders}, device_id_type=MESH)

    def x_copy(d, j):
        part = left.at[lo, chunk(j)]
        peer = hi * holders + lax.rem(lo + d, holders)
        return pltpu.make_async_remote_copy(
            src_ref=part, dst_ref=part, send_sem=x_send.at[d - 1], recv_sem=x_recv.at[d - 1, j],
            device_id={"col": peer}, device_id_type=MESH)

    def x_arrival(d, j):
        part = left.at[lax.rem(lo + holders - d, holders), chunk(j)]
        peer = hi * holders + lax.rem(lo + holders - d, holders)
        return pltpu.make_async_remote_copy(
            src_ref=part, dst_ref=part, send_sem=x_send.at[d - 1], recv_sem=x_recv.at[d - 1, j],
            device_id={"col": peer}, device_id_type=MESH)

    def r_rows(i):
        return pl.ds(pl.multiple_of(i * RIGHT, RIGHT), RIGHT)

    def r_copy(i):
        part = right.at[r_rows(i)]
        return pltpu.make_async_remote_copy(
            src_ref=part, dst_ref=part, send_sem=r_send, recv_sem=r_recv.at[i],
            device_id={"row": r + 1}, device_id_type=MESH)

    @pl.loop(0, n_adj)
    def _(i):
        adj_copy(i).start()

    barrier = pltpu.get_barrier_semaphore()

    def greet(where):
        pl.semaphore_signal(barrier, inc=1, device_id=where, device_id_type=MESH)

    @pl.when(hi > 0)
    def _():
        greet({"col": c - holders})

    @pl.when(hi < stages - 1)
    def _():
        greet({"col": c + holders})

    for d in range(1, holders):
        greet({"col": hi * holders + lax.rem(lo + d, holders)})

    @pl.when(r > 0)
    def _():
        greet({"row": r - 1})

    @pl.when(r < n_rows - 1)
    def _():
        greet({"row": r + 1})

    def convert_left(j):
        left[lo, chunk(j), :] = adj[chunk(j), :].astype(jnp.bfloat16)

    def convert_right(i):
        right[r_rows(i), :] = adj[r_rows(i), :].astype(jnp.bfloat16)

    adj_copy(0).wait()

    @pl.when(hi == 0)
    def _():
        convert_left(0)

    @pl.when(r == 0)
    def _():
        convert_right(0)

    known = ((hi > 0).astype(jnp.int32) + (hi < stages - 1).astype(jnp.int32) + (holders - 1)
             + (r > 0).astype(jnp.int32) + (r < n_rows - 1).astype(jnp.int32))
    pl.semaphore_wait(barrier, known)

    def step(j):
        @pl.when(j + 1 < n_adj)
        def _():
            adj_copy(j + 1).wait()

        @pl.when((hi == 0) & (j + 1 < n_chunks))
        def _():
            convert_left(j + 1)

        @pl.when((r == 0) & (j + 1 < n_right))
        def _():
            convert_right(j + 1)

        @pl.when(hi > 0)
        def _():
            z_copy(j).wait_recv()

        @pl.when(hi < stages - 1)
        def _():
            z_copy(j).start()

        for d in range(1, holders):
            x_copy(d, j).start()

        i = j - lag

        @pl.when((i >= 0) & (i < n_right))
        def _():
            @pl.when(r > 0)
            def _():
                r_copy(i).wait_recv()

            @pl.when(r < n_rows - 1)
            def _():
                r_copy(i).start()

    def compute(u):
        g = u // n_tiles
        t = lax.rem(u, n_tiles)

        @pl.when(t == 0)
        def _():
            for d in range(1, holders):
                @pl.loop(0, per_group)
                def _(k):
                    x_arrival(d, g * per_group + k).wait_recv()

        rows = pl.ds(pl.multiple_of(g * GROUP, GROUP), GROUP)
        cols = pl.ds(pl.multiple_of(t * TILE, TILE), TILE)
        counts = jnp.zeros((GROUP, TILE), jnp.float32)
        for h in range(holders):
            counts += jnp.dot(left[h, rows, :], right[h * block_cols:(h + 1) * block_cols, cols],
                              preferred_element_type=jnp.float32)
        out[rows, cols] = jnp.where(counts > 0.5, 1, adj[rows, cols]).astype(out.dtype)

    body_units = units - n_tiles
    ready = n_right - 1 + lag_of(n_rows - 1)
    first = min(n_chunks, max(ready, n_chunks - 2 - -(-body_units // PER_STEP)))
    done = min(body_units, PER_STEP * (n_chunks - first))
    done -= done % PER_STEP

    @pl.loop(0, first)
    def _(j):
        step(j)

    @pl.loop(first, n_chunks)
    def _(j):
        step(j)
        for p in range(PER_STEP):
            u = (j - first) * PER_STEP + p

            @pl.when(u < done)
            def _():
                compute(u)

    @pl.loop(n_chunks, max(n_chunks, ready + 1))
    def _(j):
        i = j - lag

        @pl.when((i >= 0) & (i < n_right))
        def _():
            @pl.when(r > 0)
            def _():
                r_copy(i).wait_recv()

            @pl.when(r < n_rows - 1)
            def _():
                r_copy(i).start()

    @pl.loop(done, units)
    def _(u):
        compute(u)

    whole = left.at[lo]

    @pl.when(hi < stages - 1)
    def _():
        pltpu.make_async_remote_copy(
            src_ref=whole, dst_ref=whole, send_sem=z_send, recv_sem=z_recv.at[0],
            device_id={"col": c + holders}, device_id_type=MESH).wait_send()

    for d in range(1, holders):
        pltpu.make_async_remote_copy(
            src_ref=whole, dst_ref=whole, send_sem=x_send.at[d - 1], recv_sem=x_recv.at[d - 1, 0],
            device_id={"col": hi * holders + lax.rem(lo + d, holders)}, device_id_type=MESH).wait_send()

    @pl.when(r < n_rows - 1)
    def _():
        pltpu.make_async_remote_copy(
            src_ref=right, dst_ref=right, send_sem=r_send, recv_sem=r_recv.at[0],
            device_id={"row": r + 1}, device_id_type=MESH).wait_send()


def per_device(n_rows, n_cols, adjacency):
    block_rows, block_cols = adjacency.shape
    window = PANELS * PANEL
    holders = window // block_cols
    n_chunks = block_rows // CHUNK
    dma = pltpu.SemaphoreType.DMA
    closed = pl.pallas_call(
        functools.partial(kernel, n_rows, n_cols, window),
        out_shape=pltpu.VMEM((block_rows, block_cols), jnp.bfloat16),
        in_specs=[pl.BlockSpec(memory_space=pltpu.HBM)],
        out_specs=pl.BlockSpec(memory_space=pltpu.VMEM),
        scratch_shapes=[
            pltpu.VMEM((block_rows, block_cols), jnp.int32),
            pltpu.VMEM((holders, block_rows, block_cols), jnp.bfloat16),
            pltpu.VMEM((window, block_cols), jnp.bfloat16),
            dma((block_rows // RIGHT,)),
            dma,
            dma((n_chunks,)),
            dma((holders - 1,)),
            dma((holders - 1, n_chunks)),
            dma,
            dma((window // RIGHT,)),
        ],
        compiler_params=pltpu.CompilerParams(
            collective_id=0, has_side_effects=True, vmem_limit_bytes=40 * 1024 * 1024),
    )(pltpu.with_memory_space_constraint(adjacency, pltpu.HBM))
    return closed


def solution(mesh):
    spec = P("row", "col")
    return jax.shard_map(
        functools.partial(per_device, mesh.shape["row"], mesh.shape["col"]),
        mesh=mesh, in_specs=(spec,), out_specs=spec, check_vma=False)
```

```python
import functools

import jax
import jax.numpy as jnp
from jax import lax
from jax.experimental import pallas as pl
from jax.experimental.pallas import tpu as pltpu
from jax.sharding import PartitionSpec as P

PANEL = 512
PANELS = 4

CHUNK = 32
RIGHT = 64
GROUP = 256
TAIL = 128
TILE = 256
PER_STEP = 2
MESH = pl.DeviceIdType.MESH


def lag_of(row):
    return 1 + (5 * row) // 2


def kernel(n_rows, n_cols, window, adj_hbm, out, adj, left, right, partial,
           adj_sem, z_send, z_recv, x_send, x_recv, r_send, r_recv):
    block_rows, block_cols = adj.shape
    holders = left.shape[0]
    stages = n_cols // holders
    n_chunks = block_rows // CHUNK
    n_adj = block_rows // RIGHT
    n_right = window // RIGHT
    n_groups = block_rows // GROUP
    n_tiles = block_cols // TILE
    units = n_groups * n_tiles
    per_group = GROUP // CHUNK

    r = lax.axis_index("row")
    c = lax.axis_index("col")
    hi = c // holders
    lo = lax.rem(c, holders)
    lag = lag_of(r)

    def adj_copy(i):
        rows = pl.ds(pl.multiple_of(i * RIGHT, RIGHT), RIGHT)
        return pltpu.make_async_copy(adj_hbm.at[rows], adj.at[rows], adj_sem.at[i])

    def chunk(j):
        return pl.ds(pl.multiple_of(j * CHUNK, CHUNK), CHUNK)

    def z_copy(j):
        part = left.at[lo, chunk(j)]
        return pltpu.make_async_remote_copy(
            src_ref=part, dst_ref=part, send_sem=z_send, recv_sem=z_recv.at[j],
            device_id={"col": c + holders}, device_id_type=MESH)

    def x_copy(d, j):
        part = left.at[lo, chunk(j)]
        peer = hi * holders + lax.rem(lo + d, holders)
        return pltpu.make_async_remote_copy(
            src_ref=part, dst_ref=part, send_sem=x_send.at[d - 1], recv_sem=x_recv.at[d - 1, j],
            device_id={"col": peer}, device_id_type=MESH)

    def x_arrival(d, j):
        part = left.at[lax.rem(lo + holders - d, holders), chunk(j)]
        peer = hi * holders + lax.rem(lo + holders - d, holders)
        return pltpu.make_async_remote_copy(
            src_ref=part, dst_ref=part, send_sem=x_send.at[d - 1], recv_sem=x_recv.at[d - 1, j],
            device_id={"col": peer}, device_id_type=MESH)

    def r_rows(i):
        return pl.ds(pl.multiple_of(i * RIGHT, RIGHT), RIGHT)

    def r_copy(i):
        part = right.at[r_rows(i)]
        return pltpu.make_async_remote_copy(
            src_ref=part, dst_ref=part, send_sem=r_send, recv_sem=r_recv.at[i],
            device_id={"row": r + 1}, device_id_type=MESH)

    adj_copy(0).start()

    barrier = pltpu.get_barrier_semaphore()

    def greet(where):
        pl.semaphore_signal(barrier, inc=1, device_id=where, device_id_type=MESH)

    @pl.when(hi > 0)
    def _():
        greet({"col": c - holders})

    @pl.when(hi < stages - 1)
    def _():
        greet({"col": c + holders})

    for d in range(1, holders):
        greet({"col": hi * holders + lax.rem(lo + d, holders)})

    @pl.when(r > 0)
    def _():
        greet({"row": r - 1})

    @pl.when(r < n_rows - 1)
    def _():
        greet({"row": r + 1})

    def convert_left(j):
        left[lo, chunk(j), :] = adj[chunk(j), :].astype(jnp.bfloat16)

    def convert_right(i):
        right[r_rows(i), :] = adj[r_rows(i), :].astype(jnp.bfloat16)

    ahead = RIGHT // CHUNK
    adj_copy(0).wait()

    @pl.loop(1, n_adj)
    def _(i):
        adj_copy(i).start()

    @pl.when(hi == 0)
    def _():
        for k in range(ahead):
            convert_left(k)

    @pl.when(r == 0)
    def _():
        convert_right(0)

    known = ((hi > 0).astype(jnp.int32) + (hi < stages - 1).astype(jnp.int32) + (holders - 1)
             + (r > 0).astype(jnp.int32) + (r < n_rows - 1).astype(jnp.int32))
    pl.semaphore_wait(barrier, known)

    def step(j):
        @pl.when(hi > 0)
        def _():
            z_copy(j).wait_recv()

        @pl.when(hi < stages - 1)
        def _():
            z_copy(j).start()

        for d in range(1, holders):
            x_copy(d, j).start()

        i = j - lag

        @pl.when((i >= 0) & (i < n_right))
        def _():
            @pl.when(r > 0)
            def _():
                r_copy(i).wait_recv()

            @pl.when(r < n_rows - 1)
            def _():
                r_copy(i).start()

        @pl.when(j + 1 < n_adj)
        def _():
            adj_copy(j + 1).wait()

        @pl.when((hi == 0) & (j + ahead < n_chunks))
        def _():
            convert_left(j + ahead)

        @pl.when((r == 0) & (j + 1 < n_right))
        def _():
            convert_right(j + 1)

    def compute(u):
        g = u // n_tiles
        t = lax.rem(u, n_tiles)

        @pl.when(t == 0)
        def _():
            for d in range(1, holders):
                @pl.loop(0, per_group)
                def _(k):
                    x_arrival(d, g * per_group + k).wait_recv()

        rows = pl.ds(pl.multiple_of(g * GROUP, GROUP), GROUP)
        cols = pl.ds(pl.multiple_of(t * TILE, TILE), TILE)
        counts = jnp.zeros((GROUP, TILE), jnp.float32)
        for h in range(holders):
            counts += jnp.dot(left[h, rows, :], right[h * block_cols:(h + 1) * block_cols, cols],
                              preferred_element_type=jnp.float32)
        out[rows, cols] = jnp.where(counts > 0.5, 1, adj[rows, cols]).astype(out.dtype)

    body_units = units - n_tiles
    ready = n_right - 1 + lag_of(n_rows - 1)
    first = min(n_chunks, max(ready, n_chunks - 2 - -(-body_units // PER_STEP)))
    done = min(body_units, PER_STEP * (n_chunks - first))
    done -= done % PER_STEP

    @pl.loop(0, first)
    def _(j):
        step(j)

    @pl.loop(first, n_chunks)
    def _(j):
        step(j)
        for p in range(PER_STEP):
            u = (j - first) * PER_STEP + p

            @pl.when(u < done)
            def _():
                compute(u)

    @pl.loop(n_chunks, max(n_chunks, ready + 1))
    def _(j):
        i = j - lag

        @pl.when((i >= 0) & (i < n_right))
        def _():
            @pl.when(r > 0)
            def _():
                r_copy(i).wait_recv()

            @pl.when(r < n_rows - 1)
            def _():
                r_copy(i).start()

    @pl.loop(done, body_units)
    def _(u):
        compute(u)

    def arrived(start):
        for d in range(1, holders):
            @pl.loop(start // CHUNK, (start + TAIL) // CHUNK)
            def _(k):
                x_arrival(d, k).wait_recv()

    def half(h, start, cols):
        rights = pl.ds(pl.multiple_of(h * block_cols, block_cols), block_cols)
        return jnp.dot(left[h, start:start + TAIL, :], right[rights, cols], preferred_element_type=jnp.float32)

    tiles = [slice(t * TILE, (t + 1) * TILE) for t in range(n_tiles)]
    for start in range(block_rows - GROUP, block_rows, TAIL):
        last = start + TAIL == block_rows
        if not last:
            arrived(start)
        for cols in tiles:
            partial[:, cols] = half(lo, start, cols)
        if last:
            arrived(start)
        for cols in tiles:
            counts = partial[:, cols]
            for d in range(1, holders):
                counts += half(lax.rem(lo + holders - d, holders), start, cols)
            out[start:start + TAIL, cols] = jnp.where(
                counts > 0.5, 1, adj[start:start + TAIL, cols]).astype(out.dtype)

    whole = left.at[lo]

    @pl.when(hi < stages - 1)
    def _():
        pltpu.make_async_remote_copy(
            src_ref=whole, dst_ref=whole, send_sem=z_send, recv_sem=z_recv.at[0],
            device_id={"col": c + holders}, device_id_type=MESH).wait_send()

    for d in range(1, holders):
        pltpu.make_async_remote_copy(
            src_ref=whole, dst_ref=whole, send_sem=x_send.at[d - 1], recv_sem=x_recv.at[d - 1, 0],
            device_id={"col": hi * holders + lax.rem(lo + d, holders)}, device_id_type=MESH).wait_send()

    @pl.when(r < n_rows - 1)
    def _():
        pltpu.make_async_remote_copy(
            src_ref=right, dst_ref=right, send_sem=r_send, recv_sem=r_recv.at[0],
            device_id={"row": r + 1}, device_id_type=MESH).wait_send()


def per_device(n_rows, n_cols, adjacency):
    block_rows, block_cols = adjacency.shape
    window = PANELS * PANEL
    holders = window // block_cols
    n_chunks = block_rows // CHUNK
    dma = pltpu.SemaphoreType.DMA
    closed = pl.pallas_call(
        functools.partial(kernel, n_rows, n_cols, window),
        out_shape=pltpu.VMEM((block_rows, block_cols), jnp.bfloat16),
        in_specs=[pl.BlockSpec(memory_space=pltpu.HBM)],
        out_specs=pl.BlockSpec(memory_space=pltpu.VMEM),
        scratch_shapes=[
            pltpu.VMEM((block_rows, block_cols), jnp.int32),
            pltpu.VMEM((holders, block_rows, block_cols), jnp.bfloat16),
            pltpu.VMEM((window, block_cols), jnp.bfloat16),
            pltpu.VMEM((TAIL, block_cols), jnp.float32),
            dma((block_rows // RIGHT,)),
            dma,
            dma((n_chunks,)),
            dma((holders - 1,)),
            dma((holders - 1, n_chunks)),
            dma,
            dma((window // RIGHT,)),
        ],
        compiler_params=pltpu.CompilerParams(
            collective_id=0, has_side_effects=True, vmem_limit_bytes=40 * 1024 * 1024),
    )(pltpu.with_memory_space_constraint(adjacency, pltpu.HBM))
    return closed


def solution(mesh):
    spec = P("row", "col")
    return jax.shard_map(
        functools.partial(per_device, mesh.shape["row"], mesh.shape["col"]),
        mesh=mesh, in_specs=(spec,), out_specs=spec, check_vma=False)
```

```python
import functools

import jax
import jax.numpy as jnp
from jax import lax
from jax.experimental import pallas as pl
from jax.experimental.pallas import tpu as pltpu
from jax.sharding import PartitionSpec as P

PANEL = 512
PANELS = 4

CHUNK = 32
RIGHT = 64
GROUP = 256
TAIL = 128
TILE = 256
PER_STEP = 2
MESH = pl.DeviceIdType.MESH


def lag_of(row):
    return 1 + (5 * row) // 2


def kernel(n_rows, n_cols, window, adj_hbm, out, adj, left, right, partial,
           adj_sem, z_send, b_send, z_recv, x_send, x_recv, r_send, r_recv):
    block_rows, block_cols = adj.shape
    holders = left.shape[0]
    stages = n_cols // holders
    n_chunks = block_rows // CHUNK
    n_adj = block_rows // RIGHT
    n_right = window // RIGHT
    n_groups = block_rows // GROUP
    n_tiles = block_cols // TILE
    units = n_groups * n_tiles
    per_group = GROUP // CHUNK

    r = lax.axis_index("row")
    c = lax.axis_index("col")
    hi = c // holders
    lo = lax.rem(c, holders)
    lag = lag_of(r)

    relay = lax.rem(hi, 2) == 0
    feeds_next = relay & (hi < stages - 1)
    feeds_back = relay & (hi > 0)
    next_col = c + holders * (1 + (hi + 2 < stages).astype(jnp.int32))
    back_col = c - holders

    def adj_copy(i):
        rows = pl.ds(pl.multiple_of(i * RIGHT, RIGHT), RIGHT)
        return pltpu.make_async_copy(adj_hbm.at[rows], adj.at[rows], adj_sem.at[i])

    def chunk(j):
        return pl.ds(pl.multiple_of(j * CHUNK, CHUNK), CHUNK)

    def z_copy(j):
        part = left.at[lo, chunk(j)]
        return pltpu.make_async_remote_copy(
            src_ref=part, dst_ref=part, send_sem=z_send, recv_sem=z_recv.at[j],
            device_id={"col": next_col}, device_id_type=MESH)

    def z_back(j):
        part = left.at[lo, chunk(j)]
        return pltpu.make_async_remote_copy(
            src_ref=part, dst_ref=part, send_sem=b_send, recv_sem=z_recv.at[j],
            device_id={"col": back_col}, device_id_type=MESH)

    def x_copy(d, j):
        part = left.at[lo, chunk(j)]
        peer = hi * holders + lax.rem(lo + d, holders)
        return pltpu.make_async_remote_copy(
            src_ref=part, dst_ref=part, send_sem=x_send.at[d - 1], recv_sem=x_recv.at[d - 1, j],
            device_id={"col": peer}, device_id_type=MESH)

    def x_arrival(d, j):
        part = left.at[lax.rem(lo + holders - d, holders), chunk(j)]
        peer = hi * holders + lax.rem(lo + holders - d, holders)
        return pltpu.make_async_remote_copy(
            src_ref=part, dst_ref=part, send_sem=x_send.at[d - 1], recv_sem=x_recv.at[d - 1, j],
            device_id={"col": peer}, device_id_type=MESH)

    def r_rows(i):
        return pl.ds(pl.multiple_of(i * RIGHT, RIGHT), RIGHT)

    def r_copy(i):
        part = right.at[r_rows(i)]
        return pltpu.make_async_remote_copy(
            src_ref=part, dst_ref=part, send_sem=r_send, recv_sem=r_recv.at[i],
            device_id={"row": r + 1}, device_id_type=MESH)

    adj_copy(0).start()

    barrier = pltpu.get_barrier_semaphore()

    def greet(where):
        pl.semaphore_signal(barrier, inc=1, device_id=where, device_id_type=MESH)

    @pl.when(feeds_back)
    def _():
        greet({"col": c - 2 * holders})
        greet({"col": back_col})

    @pl.when(feeds_next)
    def _():
        greet({"col": next_col})

    @pl.when(~relay & (hi < stages - 1))
    def _():
        greet({"col": c + holders})

    @pl.when(~relay & (hi == stages - 1))
    def _():
        greet({"col": c - holders})

    for d in range(1, holders):
        greet({"col": hi * holders + lax.rem(lo + d, holders)})

    @pl.when(r > 0)
    def _():
        greet({"row": r - 1})

    @pl.when(r < n_rows - 1)
    def _():
        greet({"row": r + 1})

    def convert_left(j):
        left[lo, chunk(j), :] = adj[chunk(j), :].astype(jnp.bfloat16)

    def convert_right(i):
        right[r_rows(i), :] = adj[r_rows(i), :].astype(jnp.bfloat16)

    ahead = RIGHT // CHUNK
    adj_copy(0).wait()

    @pl.loop(1, n_adj)
    def _(i):
        adj_copy(i).start()

    @pl.when(hi == 0)
    def _():
        for k in range(ahead):
            convert_left(k)

    @pl.when(r == 0)
    def _():
        convert_right(0)

    known = (2 * feeds_back.astype(jnp.int32) + feeds_next.astype(jnp.int32)
             + (~relay).astype(jnp.int32) + (holders - 1)
             + (r > 0).astype(jnp.int32) + (r < n_rows - 1).astype(jnp.int32))
    pl.semaphore_wait(barrier, known)

    def step(j):
        @pl.when(hi > 0)
        def _():
            z_copy(j).wait_recv()

        @pl.when(feeds_next)
        def _():
            z_copy(j).start()

        @pl.when(feeds_back)
        def _():
            z_back(j).start()

        for d in range(1, holders):
            x_copy(d, j).start()

        i = j - lag

        @pl.when((i >= 0) & (i < n_right))
        def _():
            @pl.when(r > 0)
            def _():
                r_copy(i).wait_recv()

            @pl.when(r < n_rows - 1)
            def _():
                r_copy(i).start()

        @pl.when(j + 1 < n_adj)
        def _():
            adj_copy(j + 1).wait()

        @pl.when((hi == 0) & (j + ahead < n_chunks))
        def _():
            convert_left(j + ahead)

        @pl.when((r == 0) & (j + 1 < n_right))
        def _():
            convert_right(j + 1)

    def compute(u):
        g = u // n_tiles
        t = lax.rem(u, n_tiles)

        @pl.when(t == 0)
        def _():
            for d in range(1, holders):
                @pl.loop(0, per_group)
                def _(k):
                    x_arrival(d, g * per_group + k).wait_recv()

        rows = pl.ds(pl.multiple_of(g * GROUP, GROUP), GROUP)
        cols = pl.ds(pl.multiple_of(t * TILE, TILE), TILE)
        counts = jnp.zeros((GROUP, TILE), jnp.float32)
        for h in range(holders):
            counts += jnp.dot(left[h, rows, :], right[h * block_cols:(h + 1) * block_cols, cols],
                              preferred_element_type=jnp.float32)
        out[rows, cols] = jnp.where(counts > 0.5, 1, adj[rows, cols]).astype(out.dtype)

    body_units = units - n_tiles
    ready = n_right - 1 + lag_of(n_rows - 1)
    first = min(n_chunks, max(ready, n_chunks - 2 - -(-body_units // PER_STEP)))
    done = min(body_units, PER_STEP * (n_chunks - first))
    done -= done % PER_STEP

    @pl.loop(0, first)
    def _(j):
        step(j)

    @pl.loop(first, n_chunks)
    def _(j):
        step(j)
        for p in range(PER_STEP):
            u = (j - first) * PER_STEP + p

            @pl.when(u < done)
            def _():
                compute(u)

    @pl.loop(n_chunks, max(n_chunks, ready + 1))
    def _(j):
        i = j - lag

        @pl.when((i >= 0) & (i < n_right))
        def _():
            @pl.when(r > 0)
            def _():
                r_copy(i).wait_recv()

            @pl.when(r < n_rows - 1)
            def _():
                r_copy(i).start()

    @pl.loop(done, body_units)
    def _(u):
        compute(u)

    def arrived(start):
        for d in range(1, holders):
            @pl.loop(start // CHUNK, (start + TAIL) // CHUNK)
            def _(k):
                x_arrival(d, k).wait_recv()

    def half(h, start, cols):
        rights = pl.ds(pl.multiple_of(h * block_cols, block_cols), block_cols)
        return jnp.dot(left[h, start:start + TAIL, :], right[rights, cols], preferred_element_type=jnp.float32)

    tiles = [slice(t * TILE, (t + 1) * TILE) for t in range(n_tiles)]
    for start in range(block_rows - GROUP, block_rows, TAIL):
        last = start + TAIL == block_rows
        if not last:
            arrived(start)
        for cols in tiles:
            partial[:, cols] = half(lo, start, cols)
        if last:
            arrived(start)
        for cols in tiles:
            counts = partial[:, cols]
            for d in range(1, holders):
                counts += half(lax.rem(lo + holders - d, holders), start, cols)
            out[start:start + TAIL, cols] = jnp.where(
                counts > 0.5, 1, adj[start:start + TAIL, cols]).astype(out.dtype)

    whole = left.at[lo]

    @pl.when(feeds_next)
    def _():
        pltpu.make_async_remote_copy(
            src_ref=whole, dst_ref=whole, send_sem=z_send, recv_sem=z_recv.at[0],
            device_id={"col": next_col}, device_id_type=MESH).wait_send()

    @pl.when(feeds_back)
    def _():
        pltpu.make_async_remote_copy(
            src_ref=whole, dst_ref=whole, send_sem=b_send, recv_sem=z_recv.at[0],
            device_id={"col": back_col}, device_id_type=MESH).wait_send()

    for d in range(1, holders):
        pltpu.make_async_remote_copy(
            src_ref=whole, dst_ref=whole, send_sem=x_send.at[d - 1], recv_sem=x_recv.at[d - 1, 0],
            device_id={"col": hi * holders + lax.rem(lo + d, holders)}, device_id_type=MESH).wait_send()

    @pl.when(r < n_rows - 1)
    def _():
        pltpu.make_async_remote_copy(
            src_ref=right, dst_ref=right, send_sem=r_send, recv_sem=r_recv.at[0],
            device_id={"row": r + 1}, device_id_type=MESH).wait_send()


def per_device(n_rows, n_cols, adjacency):
    block_rows, block_cols = adjacency.shape
    window = PANELS * PANEL
    holders = window // block_cols
    n_chunks = block_rows // CHUNK
    dma = pltpu.SemaphoreType.DMA
    closed = pl.pallas_call(
        functools.partial(kernel, n_rows, n_cols, window),
        out_shape=pltpu.VMEM((block_rows, block_cols), jnp.bfloat16),
        in_specs=[pl.BlockSpec(memory_space=pltpu.HBM)],
        out_specs=pl.BlockSpec(memory_space=pltpu.VMEM),
        scratch_shapes=[
            pltpu.VMEM((block_rows, block_cols), jnp.int32),
            pltpu.VMEM((holders, block_rows, block_cols), jnp.bfloat16),
            pltpu.VMEM((window, block_cols), jnp.bfloat16),
            pltpu.VMEM((TAIL, block_cols), jnp.float32),
            dma((block_rows // RIGHT,)),
            dma,
            dma,
            dma((n_chunks,)),
            dma((holders - 1,)),
            dma((holders - 1, n_chunks)),
            dma,
            dma((window // RIGHT,)),
        ],
        compiler_params=pltpu.CompilerParams(
            collective_id=0, has_side_effects=True, vmem_limit_bytes=40 * 1024 * 1024),
    )(pltpu.with_memory_space_constraint(adjacency, pltpu.HBM))
    return closed


def solution(mesh):
    spec = P("row", "col")
    return jax.shard_map(
        functools.partial(per_device, mesh.shape["row"], mesh.shape["col"]),
        mesh=mesh, in_specs=(spec,), out_specs=spec, check_vma=False)
```

```python
import functools

import jax
import jax.numpy as jnp
from jax import lax
from jax.experimental import pallas as pl
from jax.experimental.pallas import tpu as pltpu
from jax.sharding import PartitionSpec as P

PANEL = 512
PANELS = 4

CHUNK = 32
RIGHT = 64
GROUP = 256
TAIL = 128
TILE = 512
PER_STEP = 1
MESH = pl.DeviceIdType.MESH


def lag_of(row):
    return 1 + (5 * row) // 2


def kernel(n_rows, n_cols, window, adj_hbm, out, adj, left, right, partial,
           adj_sem, z_send, b_send, z_recv, x_send, x_recv, r_send, r_recv):
    block_rows, block_cols = adj.shape
    holders = left.shape[0]
    stages = n_cols // holders
    n_chunks = block_rows // CHUNK
    n_adj = block_rows // RIGHT
    n_right = window // RIGHT
    n_groups = block_rows // GROUP
    n_tiles = block_cols // TILE
    units = n_groups * n_tiles
    per_group = GROUP // CHUNK

    r = lax.axis_index("row")
    c = lax.axis_index("col")
    hi = c // holders
    lo = lax.rem(c, holders)
    lag = lag_of(r)

    relay = lax.rem(hi, 2) == 0
    feeds_next = relay & (hi < stages - 1)
    feeds_back = relay & (hi > 0)
    next_col = c + holders * (1 + (hi + 2 < stages).astype(jnp.int32))
    back_col = c - holders

    def adj_copy(i):
        rows = pl.ds(pl.multiple_of(i * RIGHT, RIGHT), RIGHT)
        return pltpu.make_async_copy(adj_hbm.at[rows], adj.at[rows], adj_sem.at[i])

    def chunk(j):
        return pl.ds(pl.multiple_of(j * CHUNK, CHUNK), CHUNK)

    def z_copy(j):
        part = left.at[lo, chunk(j)]
        return pltpu.make_async_remote_copy(
            src_ref=part, dst_ref=part, send_sem=z_send, recv_sem=z_recv.at[j],
            device_id={"col": next_col}, device_id_type=MESH)

    def z_back(j):
        part = left.at[lo, chunk(j)]
        return pltpu.make_async_remote_copy(
            src_ref=part, dst_ref=part, send_sem=b_send, recv_sem=z_recv.at[j],
            device_id={"col": back_col}, device_id_type=MESH)

    def x_copy(d, j):
        part = left.at[lo, chunk(j)]
        peer = hi * holders + lax.rem(lo + d, holders)
        return pltpu.make_async_remote_copy(
            src_ref=part, dst_ref=part, send_sem=x_send.at[d - 1], recv_sem=x_recv.at[d - 1, j],
            device_id={"col": peer}, device_id_type=MESH)

    def x_arrival(d, j):
        part = left.at[lax.rem(lo + holders - d, holders), chunk(j)]
        peer = hi * holders + lax.rem(lo + holders - d, holders)
        return pltpu.make_async_remote_copy(
            src_ref=part, dst_ref=part, send_sem=x_send.at[d - 1], recv_sem=x_recv.at[d - 1, j],
            device_id={"col": peer}, device_id_type=MESH)

    def r_rows(i):
        return pl.ds(pl.multiple_of(i * RIGHT, RIGHT), RIGHT)

    def r_copy(i):
        part = right.at[r_rows(i)]
        return pltpu.make_async_remote_copy(
            src_ref=part, dst_ref=part, send_sem=r_send, recv_sem=r_recv.at[i],
            device_id={"row": r + 1}, device_id_type=MESH)

    adj_copy(0).start()

    barrier = pltpu.get_barrier_semaphore()

    def greet(where):
        pl.semaphore_signal(barrier, inc=1, device_id=where, device_id_type=MESH)

    @pl.when(feeds_back)
    def _():
        greet({"col": c - 2 * holders})
        greet({"col": back_col})

    @pl.when(feeds_next)
    def _():
        greet({"col": next_col})

    @pl.when(~relay & (hi < stages - 1))
    def _():
        greet({"col": c + holders})

    @pl.when(~relay & (hi == stages - 1))
    def _():
        greet({"col": c - holders})

    for d in range(1, holders):
        greet({"col": hi * holders + lax.rem(lo + d, holders)})

    @pl.when(r > 0)
    def _():
        greet({"row": r - 1})

    @pl.when(r < n_rows - 1)
    def _():
        greet({"row": r + 1})

    def convert_left(j):
        left[lo, chunk(j), :] = adj[chunk(j), :].astype(jnp.bfloat16)

    def convert_right(i):
        right[r_rows(i), :] = adj[r_rows(i), :].astype(jnp.bfloat16)

    ahead = RIGHT // CHUNK
    adj_copy(0).wait()

    @pl.loop(1, n_adj)
    def _(i):
        adj_copy(i).start()

    @pl.when(hi == 0)
    def _():
        for k in range(ahead):
            convert_left(k)

    @pl.when(r == 0)
    def _():
        convert_right(0)

    known = (2 * feeds_back.astype(jnp.int32) + feeds_next.astype(jnp.int32)
             + (~relay).astype(jnp.int32) + (holders - 1)
             + (r > 0).astype(jnp.int32) + (r < n_rows - 1).astype(jnp.int32))
    pl.semaphore_wait(barrier, known)

    def step(j):
        @pl.when(hi > 0)
        def _():
            z_copy(j).wait_recv()

        @pl.when(feeds_next)
        def _():
            z_copy(j).start()

        @pl.when(feeds_back)
        def _():
            z_back(j).start()

        for d in range(1, holders):
            x_copy(d, j).start()

        i = j - lag

        @pl.when((i >= 0) & (i < n_right))
        def _():
            @pl.when(r > 0)
            def _():
                r_copy(i).wait_recv()

            @pl.when(r < n_rows - 1)
            def _():
                r_copy(i).start()

        @pl.when(j + 1 < n_adj)
        def _():
            adj_copy(j + 1).wait()

        @pl.when((hi == 0) & (j + ahead < n_chunks))
        def _():
            convert_left(j + ahead)

        @pl.when((r == 0) & (j + 1 < n_right))
        def _():
            convert_right(j + 1)

    def compute(u):
        g = u // n_tiles
        t = lax.rem(u, n_tiles)

        @pl.when(t == 0)
        def _():
            for d in range(1, holders):
                @pl.loop(0, per_group)
                def _(k):
                    x_arrival(d, g * per_group + k).wait_recv()

        rows = pl.ds(pl.multiple_of(g * GROUP, GROUP), GROUP)
        cols = pl.ds(pl.multiple_of(t * TILE, TILE), TILE)
        counts = jnp.zeros((GROUP, TILE), jnp.float32)
        for h in range(holders):
            counts += jnp.dot(left[h, rows, :], right[h * block_cols:(h + 1) * block_cols, cols],
                              preferred_element_type=jnp.float32)
        out[rows, cols] = jnp.where(counts > 0.5, 1, adj[rows, cols]).astype(out.dtype)

    body_units = units - n_tiles
    ready = n_right - 1 + lag_of(n_rows - 1)
    first = min(n_chunks, max(ready, n_chunks - 2 - -(-body_units // PER_STEP)))
    done = min(body_units, PER_STEP * (n_chunks - first))
    done -= done % PER_STEP

    @pl.loop(0, first)
    def _(j):
        step(j)

    @pl.loop(first, n_chunks)
    def _(j):
        step(j)
        for p in range(PER_STEP):
            u = (j - first) * PER_STEP + p

            @pl.when(u < done)
            def _():
                compute(u)

    @pl.loop(n_chunks, max(n_chunks, ready + 1))
    def _(j):
        i = j - lag

        @pl.when((i >= 0) & (i < n_right))
        def _():
            @pl.when(r > 0)
            def _():
                r_copy(i).wait_recv()

            @pl.when(r < n_rows - 1)
            def _():
                r_copy(i).start()

    @pl.loop(done, body_units)
    def _(u):
        compute(u)

    def arrived(start):
        for d in range(1, holders):
            @pl.loop(start // CHUNK, (start + TAIL) // CHUNK)
            def _(k):
                x_arrival(d, k).wait_recv()

    def half(h, start, cols):
        rights = pl.ds(pl.multiple_of(h * block_cols, block_cols), block_cols)
        return jnp.dot(left[h, start:start + TAIL, :], right[rights, cols], preferred_element_type=jnp.float32)

    tiles = [slice(t * TILE, (t + 1) * TILE) for t in range(n_tiles)]
    for start in range(block_rows - GROUP, block_rows, TAIL):
        last = start + TAIL == block_rows
        if not last:
            arrived(start)
        for cols in tiles:
            partial[:, cols] = half(lo, start, cols)
        if last:
            arrived(start)
        for cols in tiles:
            counts = partial[:, cols]
            for d in range(1, holders):
                counts += half(lax.rem(lo + holders - d, holders), start, cols)
            out[start:start + TAIL, cols] = jnp.where(
                counts > 0.5, 1, adj[start:start + TAIL, cols]).astype(out.dtype)

    whole = left.at[lo]

    @pl.when(feeds_next)
    def _():
        pltpu.make_async_remote_copy(
            src_ref=whole, dst_ref=whole, send_sem=z_send, recv_sem=z_recv.at[0],
            device_id={"col": next_col}, device_id_type=MESH).wait_send()

    @pl.when(feeds_back)
    def _():
        pltpu.make_async_remote_copy(
            src_ref=whole, dst_ref=whole, send_sem=b_send, recv_sem=z_recv.at[0],
            device_id={"col": back_col}, device_id_type=MESH).wait_send()

    for d in range(1, holders):
        pltpu.make_async_remote_copy(
            src_ref=whole, dst_ref=whole, send_sem=x_send.at[d - 1], recv_sem=x_recv.at[d - 1, 0],
            device_id={"col": hi * holders + lax.rem(lo + d, holders)}, device_id_type=MESH).wait_send()

    @pl.when(r < n_rows - 1)
    def _():
        pltpu.make_async_remote_copy(
            src_ref=right, dst_ref=right, send_sem=r_send, recv_sem=r_recv.at[0],
            device_id={"row": r + 1}, device_id_type=MESH).wait_send()


def per_device(n_rows, n_cols, adjacency):
    block_rows, block_cols = adjacency.shape
    window = PANELS * PANEL
    holders = window // block_cols
    n_chunks = block_rows // CHUNK
    dma = pltpu.SemaphoreType.DMA
    closed = pl.pallas_call(
        functools.partial(kernel, n_rows, n_cols, window),
        out_shape=pltpu.VMEM((block_rows, block_cols), jnp.bfloat16),
        in_specs=[pl.BlockSpec(memory_space=pltpu.HBM)],
        out_specs=pl.BlockSpec(memory_space=pltpu.VMEM),
        scratch_shapes=[
            pltpu.VMEM((block_rows, block_cols), jnp.int32),
            pltpu.VMEM((holders, block_rows, block_cols), jnp.bfloat16),
            pltpu.VMEM((window, block_cols), jnp.bfloat16),
            pltpu.VMEM((TAIL, block_cols), jnp.float32),
            dma((block_rows // RIGHT,)),
            dma,
            dma,
            dma((n_chunks,)),
            dma((holders - 1,)),
            dma((holders - 1, n_chunks)),
            dma,
            dma((window // RIGHT,)),
        ],
        compiler_params=pltpu.CompilerParams(
            collective_id=0, has_side_effects=True, vmem_limit_bytes=40 * 1024 * 1024),
    )(pltpu.with_memory_space_constraint(adjacency, pltpu.HBM))
    return closed


def solution(mesh):
    spec = P("row", "col")
    return jax.shard_map(
        functools.partial(per_device, mesh.shape["row"], mesh.shape["col"]),
        mesh=mesh, in_specs=(spec,), out_specs=spec, check_vma=False)
```
